32 devices in a mesh: dp: 8 (over z, core), fsdp: 4 (over y, x).
Axes of the slice: x: 2, y: 2, z: 4, core: 2. Of those that a mesh axis runs over, the one named last changes fastest.
Arguments:
- layer_input_tokens: bfloat16 [32768, 768], P(('dp', 'fsdp')), may hold values from -6 to 6
- cotangent: bfloat16 [32768, 768], P(('dp', 'fsdp')), may hold values from -6 to 6
- lengths: int32 [160], P(('dp', 'fsdp')), may hold values from 33 to 512, as said below
- query_key_value_weight: float32 [768, 2304], P(('dp', 'fsdp')), may hold values from -0.21875 to 0.21875
- output_weight: float32 [768, 768], P(('dp', 'fsdp')), may hold values from -0.875 to 0.875
- up_weight: float32 [768, 3072], P(('dp', 'fsdp')), may hold values from -0.21875 to 0.21875
- down_weight: float32 [3072, 768], P(('dp', 'fsdp')), may hold values from -0.109375 to 0.109375
- a_in: float32 [768, 40], P(('dp', 'fsdp')), may hold values from -0.21875 to 0.21875
- a_down: float32 [3072, 8], P(('dp', 'fsdp')), may hold values from -0.109375 to 0.109375
- ln_gains: float32 [2, 768], P(None, ('dp', 'fsdp')), may hold values from 0.5 to 1.5
- ln_biases: float32 [2, 768], P(None, ('dp', 'fsdp')), may hold values from -3 to 3
- adapter_b: float32 [8, 6912], replicated, may hold values from -0.3 to 0.3
- moment_one: float32 [8, 6912], replicated, may hold values from -0.72 to 0.72
- moment_two: float32 [8, 6912], replicated, may hold values from 0.005 to 0.05
Outputs:
- layer_out: bfloat16 [32768, 768], P(('dp', 'fsdp'))
- input_grad: bfloat16 [32768, 768], P(('dp', 'fsdp'))
- b_grad: float32 [8, 6912], replicated
- grad_norm: float32 [], replicated
- moment_one_new: float32 [8, 6912], replicated
- moment_two_new: float32 [8, 6912], replicated
- adapter_b_new: float32 [8, 6912], replicated
The draws below stay inside these ranges and needn't reach their ends.
Inputs may be any that keep to these rules, and one draw needn't show every extreme that they name: `lengths`: item 5 j + i lies in bucket i of its set; its length is more than half of its bucket and at most the bucket. Some item has exactly 512 valid tokens.
All inputs are finite; a program needn't handle non-finite values.
Results may differ from the reference program's by a relative error of at most 0.012.
The reference program's roundings to bfloat16 on the way count: a program that leaves them out, or rounds other values in their place, can miss the bound.
Values may be sent and summed in bfloat16 or wider, within the bound.
A program may use at most 192 MiB of HBM per device.

```python
import math
import jax
import jax.numpy as jnp
from jax import lax

D = 768
H = 12
HEAD = 64
FF = 3072
ADAPTER_RANK = 8
ITEM_LEN = 512
SETS_DEV = 1
STEP = 10
ITEMS = 160
TOKENS = 32768
BW = 6912


def draw_lengths(key, part):
    first_key, second_key = jax.random.split(key)
    which = jnp.arange(ITEMS, dtype=jnp.int32) % 5
    divisor = jnp.where(which == 0, 1, jnp.where(which == 1, 2, jnp.where(which == 2, 4, 8)))
    bucket = ITEM_LEN // divisor
    lowest = bucket // 2 + 1
    values = jax.random.randint(first_key, (ITEMS,), lowest, bucket + 1)
    chosen = 5 * jax.random.randint(second_key, (), 0, ITEMS // 5)
    return jnp.where(jnp.arange(ITEMS) == chosen, ITEM_LEN, values).astype(jnp.int32)


def steps_of(rng, extent, cuts, smallest, top_value):
    def one(dim, blocks):
        heights = jax.random.uniform(jax.random.fold_in(jax.random.fold_in(rng, 6), dim), (blocks,), jnp.float32, smallest / len(cuts), top_value / len(cuts))
        return jnp.repeat(jnp.exp(heights), extent[dim] // blocks).reshape((-1,) + (1,) * (len(extent) - dim - 1))

    level = one(*cuts[0])
    for cut in cuts[1:]:
        level = level * one(*cut)
    return level


def scatter_about(own_key, extent, spread, most, cuts=(), held_as=jnp.bfloat16):
    values = jax.random.normal(own_key, extent, jnp.float32) * spread
    if len(cuts) > 0:
        values = steps_of(own_key, extent, cuts, -0.22, 0.18) * values
    return jnp.clip(values, min=-most, max=most).astype(held_as)


def setup_inputs(seed: int = 0) -> dict:
    keys = jax.random.split(jax.random.key(seed), 15)
    layer_input_tokens = scatter_about(keys[0], (TOKENS, D), 1.0, 6.0, ((0, 32),))
    cotangent = scatter_about(keys[1], (TOKENS, D), 1.0, 6.0, ((0, 32),))
    lengths = draw_lengths(jax.random.fold_in(keys[14], 71), 0)
    query_key_value_weight = scatter_about(keys[3], (D, 3 * D), D ** -0.5, 0.21875, ((0, 32),), jnp.float32)
    output_weight = scatter_about(keys[4], (D, D), (D // 16) ** -0.5, 0.875, ((0, 32),), jnp.float32)
    up_weight = scatter_about(keys[5], (D, FF), D ** -0.5, 0.21875, ((0, 32),), jnp.float32)
    down_weight = scatter_about(keys[6], (FF, D), FF ** -0.5, 0.109375, ((0, 32),), jnp.float32)
    a_in = scatter_about(keys[7], (D, 5 * ADAPTER_RANK), D ** -0.5, 0.21875, ((0, 32),), jnp.float32)
    a_down = scatter_about(keys[8], (FF, ADAPTER_RANK), FF ** -0.5, 0.109375, ((0, 32),), jnp.float32)
    ln_gains = jnp.clip(1.0 + 0.1 * jax.random.normal(keys[9], (2, D), jnp.float32), 0.5, 1.5)
    ln_biases = scatter_about(keys[10], (2, D), 0.3, 3.0, ((1, 32),), jnp.float32)
    adapter_b = scatter_about(keys[11], (ADAPTER_RANK, BW), 0.05, 0.3, (), jnp.float32)
    moment_one = scatter_about(keys[12], (ADAPTER_RANK, BW), 0.12, 0.72, (), jnp.float32)
    moment_two = jnp.clip(jnp.exp(jax.random.uniform(keys[13], (ADAPTER_RANK, BW), jnp.float32, math.log(0.005), math.log(0.05))), 0.005, 0.05)
    return dict(layer_input_tokens=layer_input_tokens, cotangent=cotangent, lengths=lengths, query_key_value_weight=query_key_value_weight, output_weight=output_weight, up_weight=up_weight, down_weight=down_weight, a_in=a_in, a_down=a_down, ln_gains=ln_gains, ln_biases=ln_biases, adapter_b=adapter_b, moment_one=moment_one, moment_two=moment_two)


@jax.custom_vjp
def lower_rows(v):
    return lax.optimization_barrier(v.astype(jnp.bfloat16)).astype(jnp.float32)

@jax.custom_vjp
def lower_backward_rows(v):
    return v

def low_keep(v):
    return (lower_rows(v), None)

def low_pass(kept, grad):
    return (grad,)

def back_keep(v):
    return (v, None)

def back_low(kept, grad):
    return (lower_rows(grad),)
lower_rows.defvjp(low_keep, low_pass)
lower_backward_rows.defvjp(back_keep, back_low)
HIGH = lax.Precision.HIGHEST
adapter_scale = 2.0
ln_eps = 1e-05
clip_norm = 256.0
beta_one = 0.9
beta_two = 0.98
learn_rate = 0.02
decay_rate = 0.01

def bucket_plan(full):
    return ((0, full, 1, 0), (full, full // 2, 1, 1), (full * 3 // 2, full // 4, 1, 2), (full * 7 // 4, full // 8, 2, 3))

def keep_mask(lengths_set, full):
    parts = []
    for offset, size, count, first in bucket_plan(full):
        positions = jnp.arange(size, dtype=jnp.int32)
        bounds = lengths_set[:, first:first + count].astype(jnp.int32)
        mask = (positions[None, None, :] < bounds[:, :, None]).astype(jnp.float32)
        parts.append(mask.reshape(lengths_set.shape[0], count * size))
    return jnp.concatenate(parts, axis=1)

def matrix_product(left, right):
    return jnp.dot(left, right, precision=HIGH, preferred_element_type=jnp.float32)

def layer_norm(resid, gain, shift):
    center = resid - lax.optimization_barrier(jnp.mean(resid, axis=-1, keepdims=True))
    variance = lax.optimization_barrier(jnp.mean(center * center, axis=-1, keepdims=True))
    return center * lax.rsqrt(variance + ln_eps) * gain + shift

def gelu_exact(values):
    return 0.5 * values * (1.0 + jax.scipy.special.erf(values * 0.7071067811865476))

def forward_group(inputs, adapters, lengths_set, frozen):
    query_key_value_weight, output_weight, up_weight, down_weight, a_in, a_down, gains, biases = frozen
    sets = inputs.shape[0]
    span_all = 2 * ITEM_LEN
    token_rows = inputs.reshape(sets * span_all, D)
    keep = keep_mask(lengths_set, ITEM_LEN)
    b_low = lower_rows(adapters)
    query_adapter_matrix = b_low[:, :D]
    key_adapter_matrix = b_low[:, D:2 * D]
    value_adapter_matrix = b_low[:, 2 * D:3 * D]
    attention_adapter_bias = b_low[:, 3 * D:4 * D]
    upper_adapter_matrix = b_low[:, 4 * D:4 * D + FF]
    lower_adapter_matrix = b_low[:, 4 * D + FF:]
    projection_down_matrix = lower_rows(lower_backward_rows(matrix_product(token_rows, a_in[:, :3 * ADAPTER_RANK])))
    adapter_projection_delta = jnp.concatenate([matrix_product(projection_down_matrix[:, :ADAPTER_RANK], query_adapter_matrix), matrix_product(projection_down_matrix[:, ADAPTER_RANK:2 * ADAPTER_RANK], key_adapter_matrix), matrix_product(projection_down_matrix[:, 2 * ADAPTER_RANK:], value_adapter_matrix)], axis=1)
    query_key_value = lower_rows(lower_backward_rows(matrix_product(token_rows, query_key_value_weight) + adapter_scale * adapter_projection_delta))
    query_key_value = query_key_value.reshape(sets, span_all, 3, H, HEAD)
    contexts = []
    for offset, size, count, first in bucket_plan(ITEM_LEN):
        span = count * size
        part = query_key_value[:, offset:offset + span].reshape(sets * count, size, 3, H, HEAD)
        keep_block = keep[:, offset:offset + span].reshape(sets * count, size)
        scores = lower_backward_rows(jnp.einsum('gqhe,gkhe->ghqk', part[:, :, 0], part[:, :, 1], precision=HIGH) * 0.125)
        scores = jnp.where(keep_block[:, None, None, :] > 0.5, scores, -1e+30)
        probs = lower_rows(jax.nn.softmax(scores, axis=-1))
        ctx = jnp.einsum('ghqk,gkhe->gqhe', probs, part[:, :, 2], precision=HIGH)
        contexts.append(ctx.reshape(sets, span, D))
    context_rows = jnp.concatenate(contexts, axis=1).reshape(sets * span_all, D)
    context_rows = lower_rows(lower_backward_rows(context_rows))
    attention_down_matrix = lower_rows(lower_backward_rows(matrix_product(context_rows, a_in[:, 3 * ADAPTER_RANK:4 * ADAPTER_RANK])))
    attention_output = lower_backward_rows(matrix_product(context_rows, output_weight) + adapter_scale * matrix_product(attention_down_matrix, attention_adapter_bias))
    hidden_one = layer_norm(token_rows + attention_output, gains[0], biases[0])
    hidden_lower_rows = lower_rows(hidden_one)
    upper_down_matrix = lower_rows(lower_backward_rows(matrix_product(hidden_lower_rows, a_in[:, 4 * ADAPTER_RANK:])))
    upper_rows = lower_backward_rows(matrix_product(hidden_lower_rows, up_weight) + adapter_scale * matrix_product(upper_down_matrix, upper_adapter_matrix))
    active_rows = lower_rows(gelu_exact(upper_rows))
    lower_down_matrix = lower_rows(lower_backward_rows(matrix_product(active_rows, a_down)))
    feedforward_output = lower_backward_rows(matrix_product(active_rows, down_weight) + adapter_scale * matrix_product(lower_down_matrix, lower_adapter_matrix))
    output = layer_norm(hidden_one + feedforward_output, gains[1], biases[1])
    return (output * keep.reshape(-1, 1)).reshape(sets, span_all, D)

def reference(layer_input_tokens, cotangent, lengths, query_key_value_weight, output_weight, up_weight, down_weight, a_in, a_down, ln_gains, ln_biases, adapter_b, moment_one, moment_two):
    frozen = (lower_rows(query_key_value_weight), lower_rows(output_weight), lower_rows(up_weight), lower_rows(down_weight), lower_rows(a_in), lower_rows(a_down), lower_rows(ln_gains), lower_rows(ln_biases))
    span_all = 2 * ITEM_LEN
    count = TOKENS // (span_all * SETS_DEV)
    inputs = layer_input_tokens.astype(jnp.float32).reshape(count, SETS_DEV, span_all, D)
    grads_in = cotangent.astype(jnp.float32).reshape(count, SETS_DEV, span_all, D)
    lengths_all = lengths.astype(jnp.int32).reshape(count, SETS_DEV, 5)

    def one_group(total, item):
        group_x, group_cot, group_len = item

        def local_forward(inputs_here, adapters_here):
            return forward_group(inputs_here, adapters_here, group_len, frozen)
        output, pull = jax.vjp(local_forward, group_x, adapter_b)
        grad_x, grad_b = pull(group_cot)
        return (total + grad_b, (output.astype(jnp.bfloat16), grad_x.astype(jnp.bfloat16)))
    b_grad, (outputs, grads) = lax.scan(one_group, jnp.zeros_like(adapter_b), (inputs, grads_in, lengths_all))
    layer_out = outputs.reshape(TOKENS, D)
    input_grad = grads.reshape(TOKENS, D)
    grad_norm = jnp.sqrt(jnp.sum(b_grad * b_grad))
    clipped = b_grad * jnp.minimum(1.0, clip_norm / (grad_norm + 1e-06))
    moment_one_new = beta_one * moment_one + (1.0 - beta_one) * clipped
    moment_two_new = beta_two * moment_two + (1.0 - beta_two) * clipped * clipped
    first_hat = moment_one_new / (1.0 - beta_one ** STEP)
    second_hat = moment_two_new / (1.0 - beta_two ** STEP)
    adapter_b_new = adapter_b - learn_rate * (first_hat / (jnp.sqrt(second_hat) + 1e-08) + decay_rate * adapter_b)
    return (layer_out, input_grad, b_grad, grad_norm, moment_one_new, moment_two_new, adapter_b_new)
```

```python
import functools
import math
import jax
import jax.numpy as jnp
from jax import lax
from jax.experimental import pallas as pl
from jax.experimental.pallas import tpu as pltpu

from jax.sharding import PartitionSpec as P


HEAD = 64
ITEM_LEN = 512
STEP = 10


adapter_scale = 2.0
ln_eps = 1e-05
clip_norm = 256.0
beta_one = 0.9
beta_two = 0.98
learn_rate = 0.02
decay_rate = 0.01


def bucket_plan(full):
    return (
        (0, full, 1, 0),
        (full, full // 2, 1, 1),
        (full * 3 // 2, full // 4, 1, 2),
        (full * 7 // 4, full // 8, 2, 3),
    )


def keep_mask(lengths_set, full):
    parts = []
    for offset, size, count, first in bucket_plan(full):
        positions = jnp.arange(size, dtype=jnp.int32)
        bounds = lengths_set[:, first : first + count]
        mask = (positions[None, None, :] < bounds[:, :, None]).astype(jnp.float32)
        parts.append(mask.reshape(lengths_set.shape[0], count * size))
    return jnp.concatenate(parts, axis=1)


def product_result(left, right):
    return jnp.dot(left, right, preferred_element_type=jnp.float32)


def transposed_product(left, right):
    return lax.dot_general(
        left, right, (((1,), (1,)), ((), ())), preferred_element_type=jnp.float32
    )


def product_tn(left, right):
    return lax.dot_general(
        left, right, (((0,), (0,)), ((), ())), preferred_element_type=jnp.float32
    )


def norm_forward(resid, gain, shift):
    center = resid - jnp.mean(resid, axis=1, keepdims=True)
    variance = jnp.mean(center * center, axis=1, keepdims=True)
    inv_std = lax.rsqrt(variance + ln_eps)
    normed = center * inv_std
    return (normed * gain + shift, normed, inv_std)


def norm_backward(grad_out, normed, inv_std, gain):
    scaled = grad_out * gain
    return inv_std * (
        scaled
        - jnp.mean(scaled, axis=1, keepdims=True)
        - normed * jnp.mean(scaled * normed, axis=1, keepdims=True)
    )


def gelu_exact(values):
    return 0.5 * values * (1.0 + jax.scipy.special.erf(values * 0.7071067811865476))


def gelu_slope(values):
    normal_cdf = 0.5 * (1.0 + jax.scipy.special.erf(values * 0.7071067811865476))
    density = jnp.exp(-0.5 * values * values) * 0.3989422804014327
    return normal_cdf + values * density


def masked_scores(query, key_rows, keep_block):
    scores = (
        jnp.einsum("gqhe,gkhe->ghqk", query, key_rows, preferred_element_type=jnp.float32) * 0.125
    )
    return jnp.where(keep_block[:, None, None, :] > 0.5, scores, -1e30)


def bucket_forward(query, key_rows, value_rows, keep_block):
    scores = masked_scores(query, key_rows, keep_block)
    highest = jnp.max(scores, axis=-1, keepdims=True)
    expo = jnp.exp(scores - highest)
    totals = jnp.sum(expo, axis=-1, keepdims=True)
    probs = (expo / totals).astype(jnp.bfloat16)
    context_rows = jnp.einsum(
        "ghqk,gkhe->gqhe", probs, value_rows, preferred_element_type=jnp.float32
    )
    return (context_rows.astype(jnp.bfloat16), highest + jnp.log(totals))


def bucket_backward(query, key_rows, value_rows, keep_block, log_total, grad_ctx):
    scores = masked_scores(query, key_rows, keep_block)
    probs = jnp.exp(scores - log_total)
    grad_probs = jnp.einsum(
        "gqhe,gkhe->ghqk", grad_ctx, value_rows, preferred_element_type=jnp.float32
    )
    delta = jnp.sum(probs * grad_probs, axis=-1, keepdims=True)
    grad_scores = (probs * (grad_probs - delta)).astype(jnp.bfloat16)
    grad_query = (
        jnp.einsum("ghqk,gkhe->gqhe", grad_scores, key_rows, preferred_element_type=jnp.float32)
        * 0.125
    )
    grad_key = (
        jnp.einsum("ghqk,gqhe->gkhe", grad_scores, query, preferred_element_type=jnp.float32)
        * 0.125
    )
    grad_value = jnp.einsum(
        "ghqk,gqhe->gkhe", probs.astype(jnp.bfloat16), grad_ctx, preferred_element_type=jnp.float32
    )
    return (
        grad_query.astype(jnp.bfloat16),
        grad_key.astype(jnp.bfloat16),
        grad_value.astype(jnp.bfloat16),
    )


def set_forward(operands):
    query, key_rows, value_rows, lens = operands
    heads, size_head = (query.shape[1], query.shape[2])
    keep_set = keep_mask(lens[None, :], ITEM_LEN)[0]
    contexts = []
    totals = []
    for offset, size, count, first in bucket_plan(ITEM_LEN):
        span = count * size
        shape = (count, size, heads, size_head)
        context_rows, log_total = bucket_forward(
            query[offset : offset + span].reshape(shape),
            key_rows[offset : offset + span].reshape(shape),
            value_rows[offset : offset + span].reshape(shape),
            keep_set[offset : offset + span].reshape(count, size),
        )
        contexts.append(context_rows.reshape(span, heads, size_head))
        totals.append(log_total)
    return (jnp.concatenate(contexts, axis=0), tuple(totals))


def set_backward(operands):
    query, key_rows, value_rows, lens, log_totals, grad_ctx = operands
    heads, size_head = (query.shape[1], query.shape[2])
    keep_set = keep_mask(lens[None, :], ITEM_LEN)[0]
    grads_q = []
    grads_k = []
    grads_v = []
    for index, (offset, size, count, first) in enumerate(bucket_plan(ITEM_LEN)):
        span = count * size
        shape = (count, size, heads, size_head)
        grad_q, grad_k, grad_v = bucket_backward(
            query[offset : offset + span].reshape(shape),
            key_rows[offset : offset + span].reshape(shape),
            value_rows[offset : offset + span].reshape(shape),
            keep_set[offset : offset + span].reshape(count, size),
            log_totals[index],
            grad_ctx[offset : offset + span].reshape(shape),
        )
        grads_q.append(grad_q.reshape(span, heads, size_head))
        grads_k.append(grad_k.reshape(span, heads, size_head))
        grads_v.append(grad_v.reshape(span, heads, size_head))
    return (
        jnp.concatenate(grads_q, axis=0),
        jnp.concatenate(grads_k, axis=0),
        jnp.concatenate(grads_v, axis=0),
    )


def adam_update(gradient, grad_norm, moment_old, second_old, weights):
    clipped = gradient * jnp.minimum(1.0, clip_norm / (grad_norm + 1e-06))
    moment_new = beta_one * moment_old + (1.0 - beta_one) * clipped
    second_new = beta_two * second_old + (1.0 - beta_two) * clipped * clipped
    first_hat = moment_new / (1.0 - beta_one**STEP)
    second_hat = second_new / (1.0 - beta_two**STEP)
    weights_new = weights - learn_rate * (
        first_hat / (jnp.sqrt(second_hat) + 1e-08) + decay_rate * weights
    )
    return (moment_new, second_new, weights_new)


MESH = pl.DeviceIdType.MESH


def grid_sizes(mesh):
    outer, inner = mesh.shape["dp"], mesh.shape["fsdp"]
    side = math.isqrt(inner)
    return (outer // 2, 2, inner // side, side)


def gather_kernel(sizes, splits, count, *refs):
    nz, nc, ny, nx = sizes
    own = refs[:count]
    full = refs[count : 2 * count]
    copy_sem, send_sem, z_sem, a_sem, b_sem, c_sem = refs[2 * count :]
    dp, fs = lax.axis_index("dp"), lax.axis_index("fsdp")
    z, core = dp // nc, lax.rem(dp, nc)
    y, x = fs // nx, lax.rem(fs, nx)

    def device(zz, cc, yy, xx):
        return (zz * nc + cc, yy * nx + xx)

    def slot(zz, cc, yy, xx):
        return (zz * nc + cc) * (ny * nx) + yy * nx + xx

    def zs(k):
        return lax.rem(z + k, nz)

    def ys(k):
        return lax.rem(y + k, ny)

    def xs(k):
        return lax.rem(x + k, nx)

    partners = (
        [(zs(k), core, y, x) for k in range(1, nz)]
        + [(z, core, ys(k), x) for k in range(1, ny)]
        + [(z, core, y, xs(k)) for k in range(1, nx)]
        + [(z, 1 - core, y, x)]
    )
    barrier = pltpu.get_barrier_semaphore()
    for other in partners:
        pl.semaphore_signal(barrier, inc=1, device_id=device(*other), device_id_type=MESH)
    pl.semaphore_wait(barrier, len(partners))

    chunks = []
    for p in range(count):
        rows, cols = own[p].shape
        for lo, hi in splits[p]:
            chunks.append((p, lo, hi))
    total = len(chunks)
    sent = [[] for _ in range(total)]

    def view(c, where):
        p, lo, hi = chunks[c]
        return full[p].at[where, :, lo:hi]

    def send(c, src, where, target, sem):
        copy = pltpu.make_async_remote_copy(
            src_ref=src,
            dst_ref=view(c, where),
            send_sem=send_sem.at[c],
            recv_sem=sem,
            device_id=device(*target),
            device_id_type=MESH,
        )
        copy.start()
        sent[c].append(copy)

    def wait_in(c, times, sem):
        if times > 0:
            bytes_of = view(c, pl.ds(0, times))
            pltpu.make_async_copy(bytes_of, bytes_of, sem).wait()

    me = slot(z, core, y, x)
    local = []
    for c in range(total):
        p, lo, hi = chunks[c]
        mine = own[p].at[:, lo:hi]
        for k in range(1, nz):
            send(c, mine, me, (zs(k), core, y, x), z_sem.at[c])
    for c in range(total):
        p, lo, hi = chunks[c]
        mine = own[p].at[:, lo:hi]
        copy = pltpu.make_async_copy(mine, view(c, me), copy_sem.at[c])
        copy.start()
        local.append(copy)

    def first(c):
        wait_in(c, nz - 1, z_sem.at[c])
        local[c].wait()
        for zz in range(nz):
            where = slot(zz, core, y, x)
            if zz % 2 == 0:
                for k in range(1, nx):
                    send(c, view(c, where), where, (z, core, y, xs(k)), a_sem.at[c])
            else:
                for k in range(1, ny):
                    send(c, view(c, where), where, (z, core, ys(k), x), a_sem.at[c])
            send(c, view(c, where), where, (z, 1 - core, y, x), c_sem.at[c])

    def second(c):
        even, odd = (nz + 1) // 2, nz // 2
        wait_in(c, even * (nx - 1) + odd * (ny - 1), a_sem.at[c])
        for zz in range(nz):
            if zz % 2 == 0:
                for i in range(nx):
                    where = slot(zz, core, y, xs(i))
                    for k in range(1, ny):
                        send(c, view(c, where), where, (z, core, ys(k), x), b_sem.at[c])
                    if i > 0:
                        send(c, view(c, where), where, (z, 1 - core, y, x), c_sem.at[c])
            else:
                for i in range(ny):
                    where = slot(zz, core, ys(i), x)
                    for k in range(1, nx):
                        send(c, view(c, where), where, (z, core, y, xs(k)), b_sem.at[c])
                    if i > 0:
                        send(c, view(c, where), where, (z, 1 - core, y, x), c_sem.at[c])

    def third(c):
        even, odd = (nz + 1) // 2, nz // 2
        wait_in(c, even * nx * (ny - 1) + odd * ny * (nx - 1), b_sem.at[c])
        for zz in range(nz):
            for i in range(nx):
                for j in range(1, ny):
                    if zz % 2 == 0:
                        where = slot(zz, core, ys(j), xs(i))
                        send(c, view(c, where), where, (z, 1 - core, y, x), c_sem.at[c])
            for i in range(1, nx):
                for j in range(ny):
                    if zz % 2 == 1:
                        where = slot(zz, core, ys(j), xs(i))
                        send(c, view(c, where), where, (z, 1 - core, y, x), c_sem.at[c])

    for step in range(total + 2):
        if step < total:
            first(step)
        if 0 <= step - 1 < total:
            second(step - 1)
        if 0 <= step - 2 < total:
            third(step - 2)
    for c in range(total):
        wait_in(c, nz * ny * nx, c_sem.at[c])
        wait_in(c, len(sent[c]), send_sem.at[c])


def gather_all(mesh, shards, splits):
    sizes = grid_sizes(mesh)
    devices = mesh.shape["dp"] * mesh.shape["fsdp"]
    count = len(shards)
    total = sum(len(s) for s in splits)
    return pl.pallas_call(
        functools.partial(gather_kernel, sizes, splits, count),
        out_shape=[jax.ShapeDtypeStruct((devices, *s.shape), s.dtype) for s in shards],
        in_specs=[pl.BlockSpec(memory_space=pltpu.VMEM)] * count,
        out_specs=[pl.BlockSpec(memory_space=pltpu.HBM)] * count,
        scratch_shapes=[pltpu.SemaphoreType.DMA((total,))] * 6,
        compiler_params=pltpu.CompilerParams(collective_id=0, has_side_effects=True),
        name="gather_weights",
    )(*shards)


def reduce_kernel(sizes, part_ref, one_ref, two_ref, low_ref, grad_ref, norm_ref, m_ref, v_ref, w_ref,
                  work, done, rbuf, cbuf, zbuf, send_sem, r_sem, c_sem, z_sem, d_sem, e_sem, *, step_fn):
    nz, nc, ny, nx = sizes
    nf = ny * nx
    dp, fs = lax.axis_index("dp"), lax.axis_index("fsdp")
    z, core = dp // nc, lax.rem(dp, nc)
    lanes = one_ref.shape[1]
    wide = work.shape[1]
    piece = wide // nf
    half = piece // 2

    barrier = pltpu.get_barrier_semaphore()
    others_f = [lax.rem(fs + k, nf) for k in range(1, nf)]
    others_z = [lax.rem(z + k, nz) for k in range(1, nz)]
    partners = [(dp, f) for f in others_f] + [(zz * nc + core, fs) for zz in others_z]
    partners.append((z * nc + 1 - core, fs))
    for other in partners:
        pl.semaphore_signal(barrier, inc=1, device_id=other, device_id_type=MESH)
    pl.semaphore_wait(barrier, len(partners))

    def remote(src, dst, s, r, target):
        copy = pltpu.make_async_remote_copy(
            src_ref=src, dst_ref=dst, send_sem=s, recv_sem=r, device_id=target, device_id_type=MESH
        )
        copy.start()
        return copy

    def lane(start, size):
        return pl.ds(pl.multiple_of(start, 128), size)

    def drain(ref, sem):
        pltpu.make_async_copy(ref, ref, sem).wait()

    pending = []
    for k in range(1, nf):
        f = lax.rem(fs + k, nf)
        pending.append(
            remote(part_ref.at[:, lane(f * piece, piece)], rbuf.at[nf - k], send_sem.at[0], r_sem, (dp, f))
        )
    drain(rbuf.at[pl.ds(1, nf - 1)], r_sem)
    mine = part_ref[:, lane(fs * piece, piece)]
    total = mine
    for k in range(1, nf):
        total = total + rbuf[k]
    work[:, lane(fs * piece, piece)] = total
    sib = (z * nc + 1 - core, fs)
    base = fs * piece
    send_half = remote(
        work.at[:, lane(base + (1 - core) * half, half)], cbuf, send_sem.at[1], c_sem, sib
    )
    send_half.wait_recv()
    keep = lane(base + core * half, half)
    zbuf[z] = work[:, keep] + cbuf[...]
    zs = []
    for k in range(1, nz):
        zz = lax.rem(z + k, nz)
        zs.append(remote(zbuf.at[z], zbuf.at[z], send_sem.at[2], z_sem, (zz * nc + core, fs)))
    drain(zbuf.at[pl.ds(0, nz - 1)], z_sem)
    total = zbuf[0]
    for k in range(1, nz):
        total = total + zbuf[k]
    done[:, keep] = total
    back = remote(done.at[:, keep], done.at[:, keep], send_sem.at[3], d_sem, sib)
    back.wait_recv()
    whole = lane(base, piece)
    outs = []
    for k in range(1, nf):
        f = lax.rem(fs + k, nf)
        outs.append(remote(done.at[:, whole], done.at[:, whole], send_sem.at[4], e_sem, (dp, f)))
    rest = pl.ds(0, (nf - 1) * piece)
    drain(done.at[:, rest], e_sem)
    drain(done.at[:, rest], send_sem.at[0])
    send_half.wait_send()
    drain(zbuf.at[pl.ds(0, nz - 1)], send_sem.at[2])
    back.wait_send()
    drain(done.at[:, rest], send_sem.at[4])
    gradient = done[:, :lanes]
    step_fn(gradient, one_ref, two_ref, low_ref, grad_ref, norm_ref, m_ref, v_ref, w_ref)


def reduce_and_step(mesh, part, one, two, weights, step_fn):
    sizes = grid_sizes(mesh)
    nz, nc, ny, nx = sizes
    nf = ny * nx
    low, lanes = one.shape
    unit = 128 * nf * 2
    wide = pl.cdiv(lanes, unit) * unit
    part = jnp.pad(part, ((0, 0), (0, wide - part.shape[1])))
    piece = wide // nf
    f32 = jnp.float32
    sd = jax.ShapeDtypeStruct
    vmem = pl.BlockSpec(memory_space=pltpu.VMEM)
    return pl.pallas_call(
        functools.partial(reduce_kernel, sizes, step_fn=step_fn),
        out_shape=[sd((low, lanes), f32), sd((1, 1), f32)] + [sd((low, lanes), f32)] * 3,
        in_specs=[vmem] * 4,
        out_specs=[vmem] * 5,
        scratch_shapes=[
            pltpu.VMEM((low, wide), f32),
            pltpu.VMEM((low, wide), f32),
            pltpu.VMEM((nf, low, piece), f32),
            pltpu.VMEM((low, piece // 2), f32),
            pltpu.VMEM((nz, low, piece // 2), f32),
            pltpu.SemaphoreType.DMA((5,)),
            pltpu.SemaphoreType.DMA,
            pltpu.SemaphoreType.DMA,
            pltpu.SemaphoreType.DMA,
            pltpu.SemaphoreType.DMA,
            pltpu.SemaphoreType.DMA,
        ],
        compiler_params=pltpu.CompilerParams(collective_id=1, has_side_effects=True),
        name="reduce_step",
    )(part, one, two, weights)


def optimizer_step(gradient, one_ref, two_ref, low_ref, grad_ref, norm_ref, m_ref, v_ref, w_ref):
    norm = jnp.sqrt(jnp.sum(gradient * gradient, axis=(0, 1), keepdims=True))
    moment_new, second_new, weights_new = adam_update(
        gradient, norm, one_ref[...], two_ref[...], low_ref[...]
    )
    grad_ref[...] = gradient
    norm_ref[...] = norm
    m_ref[...] = moment_new
    v_ref[...] = second_new
    w_ref[...] = weights_new


def on_device(
    mesh,
    layer_input_tokens,
    cotangent,
    lengths,
    query_key_value_weight,
    output_weight,
    up_weight,
    down_weight,
    a_in,
    a_down,
    ln_gains,
    ln_biases,
    adapter_b,
    moment_one,
    moment_two,
):
    total_rows, width = layer_input_tokens.shape
    span_all = 2 * ITEM_LEN
    sets = total_rows // span_all
    lowrank = adapter_b.shape[0]
    hidden = up_weight.shape[1]
    head_count = width // HEAD
    brain_float_type = jnp.bfloat16
    low = lambda value: value.astype(brain_float_type)
    rows = query_key_value_weight.shape[0]
    extra = jnp.concatenate(
        [a_in, ln_gains.T, ln_biases.T, a_down.reshape(rows, -1)], axis=1
    )
    extra = jnp.pad(extra, ((0, 0), (0, 128 - extra.shape[1])))
    first = low(jnp.concatenate([query_key_value_weight, extra], axis=1))
    g_first, g_out, g_up, g_down = gather_all(
        mesh,
        (first, low(output_weight), low(up_weight), low(down_weight)),
        (((0, 1280), (1280, 2432)), ((0, 768),), ((0, 1536), (1536, 3072)), ((0, 384), (384, 768))),
    )
    g_first = g_first.reshape(width, -1)
    projection_weight_gradient = g_first[:, : 3 * width]
    output_weight_gradient = g_out.reshape(width, width)
    up_weight_gradient = g_up.reshape(width, hidden)
    down_weight_gradient = g_down.reshape(hidden, width)
    tail = g_first[:, 3 * width :]
    five = 5 * lowrank
    g_ain = tail[:, :five]
    g_gain = tail[:, five : five + 2].T
    g_bias = tail[:, five + 2 : five + 4].T
    g_adown = tail[:, five + 4 : five + 4 + hidden * lowrank // width].reshape(hidden, lowrank)
    gain_full = g_gain.astype(jnp.float32)
    bias_full = g_bias.astype(jnp.float32)
    lengths_set = lengths.reshape(sets, 5)
    keep = keep_mask(lengths_set, ITEM_LEN)
    keep_rows = keep.reshape(-1, 1)
    b_low = adapter_b.astype(brain_float_type)
    query_adapter_matrix = b_low[:, :width]
    key_adapter_matrix = b_low[:, width : 2 * width]
    value_adapter_matrix = b_low[:, 2 * width : 3 * width]
    attention_adapter_bias = b_low[:, 3 * width : 4 * width]
    upper_adapter_matrix = b_low[:, 4 * width : 4 * width + hidden]
    lower_adapter_matrix = b_low[:, 4 * width + hidden :]
    projection_down_matrix = product_result(layer_input_tokens, g_ain[:, : 3 * lowrank]).astype(
        brain_float_type
    )
    adapter_projection_delta = jnp.concatenate(
        [
            product_result(projection_down_matrix[:, :lowrank], query_adapter_matrix),
            product_result(projection_down_matrix[:, lowrank : 2 * lowrank], key_adapter_matrix),
            product_result(projection_down_matrix[:, 2 * lowrank :], value_adapter_matrix),
        ],
        axis=1,
    )
    query_key_value = (
        product_result(layer_input_tokens, projection_weight_gradient)
        + adapter_scale * adapter_projection_delta
    ).astype(brain_float_type)
    qkv_heads = query_key_value.reshape(sets, span_all, 3, head_count, HEAD)
    query = qkv_heads[:, :, 0]
    key_rows = qkv_heads[:, :, 1]
    value_rows = qkv_heads[:, :, 2]
    context_rows, log_totals = lax.map(set_forward, (query, key_rows, value_rows, lengths_set))
    context_token_rows = context_rows.reshape(sets * span_all, width)
    attention_down_matrix = product_result(
        context_token_rows, g_ain[:, 3 * lowrank : 4 * lowrank]
    ).astype(brain_float_type)
    attention_output = product_result(
        context_token_rows, output_weight_gradient
    ) + adapter_scale * product_result(attention_down_matrix, attention_adapter_bias)
    hidden_one, normed_one, inv_one = norm_forward(
        layer_input_tokens.astype(jnp.float32) + attention_output, gain_full[0], bias_full[0]
    )
    hidden_lower_rows = hidden_one.astype(brain_float_type)
    upper_down_matrix = product_result(hidden_lower_rows, g_ain[:, 4 * lowrank :]).astype(
        brain_float_type
    )
    upper_rows = product_result(
        hidden_lower_rows, up_weight_gradient
    ) + adapter_scale * product_result(upper_down_matrix, upper_adapter_matrix)
    active_rows = gelu_exact(upper_rows).astype(brain_float_type)
    lower_down_matrix = product_result(active_rows, g_adown).astype(brain_float_type)
    feedforward_output = product_result(
        active_rows, down_weight_gradient
    ) + adapter_scale * product_result(lower_down_matrix, lower_adapter_matrix)
    output, normed_two, inv_two = norm_forward(
        hidden_one + feedforward_output, gain_full[1], bias_full[1]
    )
    layer_out = (output * keep_rows).astype(brain_float_type)
    grad_out = cotangent.astype(jnp.float32) * keep_rows
    grad_two = norm_backward(grad_out, normed_two, inv_two, gain_full[1])
    feedforward_gradient = grad_two.astype(brain_float_type)
    lower_down_gradient = (
        adapter_scale * transposed_product(feedforward_gradient, lower_adapter_matrix)
    ).astype(brain_float_type)
    grad_active = transposed_product(
        feedforward_gradient, down_weight_gradient
    ) + transposed_product(lower_down_gradient, g_adown)
    upper_output_gradient = (grad_active * gelu_slope(upper_rows)).astype(brain_float_type)
    upper_down_gradient = (
        adapter_scale * transposed_product(upper_output_gradient, upper_adapter_matrix)
    ).astype(brain_float_type)
    grad_hidden = (
        grad_two
        + transposed_product(upper_output_gradient, up_weight_gradient)
        + transposed_product(upper_down_gradient, g_ain[:, 4 * lowrank :])
    )
    grad_one = norm_backward(grad_hidden, normed_one, inv_one, gain_full[0])
    attention_gradient = grad_one.astype(brain_float_type)
    attention_down_gradient = (
        adapter_scale * transposed_product(attention_gradient, attention_adapter_bias)
    ).astype(brain_float_type)
    grad_ctx = (
        transposed_product(attention_gradient, output_weight_gradient)
        + transposed_product(attention_down_gradient, g_ain[:, 3 * lowrank : 4 * lowrank])
    ).astype(brain_float_type)
    grad_q, grad_k, grad_v = lax.map(
        set_backward,
        (
            query,
            key_rows,
            value_rows,
            lengths_set,
            log_totals,
            grad_ctx.reshape(sets, span_all, head_count, HEAD),
        ),
    )
    grad_qkv = jnp.stack([grad_q, grad_k, grad_v], axis=2).reshape(sets * span_all, 3 * width)
    grad_uqkv = (
        adapter_scale
        * jnp.concatenate(
            [
                transposed_product(grad_qkv[:, :width], query_adapter_matrix),
                transposed_product(grad_qkv[:, width : 2 * width], key_adapter_matrix),
                transposed_product(grad_qkv[:, 2 * width :], value_adapter_matrix),
            ],
            axis=1,
        )
    ).astype(brain_float_type)
    input_grad = (
        grad_one
        + transposed_product(grad_qkv, projection_weight_gradient)
        + transposed_product(grad_uqkv, g_ain[:, : 3 * lowrank])
    ).astype(brain_float_type)
    local_gradient = adapter_scale * jnp.concatenate(
        [
            product_tn(projection_down_matrix[:, :lowrank], grad_qkv[:, :width]),
            product_tn(
                projection_down_matrix[:, lowrank : 2 * lowrank], grad_qkv[:, width : 2 * width]
            ),
            product_tn(projection_down_matrix[:, 2 * lowrank :], grad_qkv[:, 2 * width :]),
            product_tn(attention_down_matrix, attention_gradient),
            product_tn(upper_down_matrix, upper_output_gradient),
            product_tn(lower_down_matrix, feedforward_gradient),
        ],
        axis=1,
    )
    b_grad, grad_norm, moment_new, second_new, adapter_new = reduce_and_step(
        mesh, local_gradient, moment_one, moment_two, adapter_b, optimizer_step
    )
    grad_norm = grad_norm.reshape(())
    return (layer_out, input_grad, b_grad, grad_norm, moment_new, second_new, adapter_new)


def solution(mesh):
    placed = (
        P(("dp", "fsdp"), None),
        P(("dp", "fsdp"), None),
        P(("dp", "fsdp")),
        P(("dp", "fsdp"), None),
        P(("dp", "fsdp"), None),
        P(("dp", "fsdp"), None),
        P(("dp", "fsdp"), None),
        P(("dp", "fsdp"), None),
        P(("dp", "fsdp"), None),
        P(None, ("dp", "fsdp")),
        P(None, ("dp", "fsdp")),
        P(),
        P(),
        P(),
    )
    return jax.shard_map(
        functools.partial(on_device, mesh),
        mesh=mesh,
        in_specs=placed,
        out_specs=(P(("dp", "fsdp"), None), P(("dp", "fsdp"), None), P(), P(), P(), P(), P()),
        check_vma=False,
    )
```
